32 devices in a mesh: data: 1 (over z), stage: 32 (over y, x, core).
Axes of the slice: x: 4, y: 4, z: 1, core: 2. Of those that a mesh axis runs over, the one named last changes fastest.
The devices are a block of a 4x4x8 slice.
Arguments:
- x_enc: bfloat16 [512, 256, 1024], P(('data', 'stage'))
- enc_len: int32 [512], P(('data', 'stage'))
- y: bfloat16 [512, 64, 1024], P(('data', 'stage'))
- enc_wqkv: bfloat16 [2, 1024, 3, 16, 128], replicated
- enc_wo: bfloat16 [2, 16, 128, 1024], replicated
- enc_w1: bfloat16 [2, 1024, 3072], replicated
- enc_w2: bfloat16 [2, 3072, 1024], replicated
- dec_wqkv: bfloat16 [2, 1024, 3, 16, 128], replicated
- dec_wo: bfloat16 [2, 16, 128, 1024], replicated
- cross_wq: bfloat16 [2, 1024, 8, 2, 128], replicated
- cross_wkv: bfloat16 [2, 1024, 2, 8, 128], replicated
- cross_wo: bfloat16 [2, 8, 2, 128, 1024], replicated
- dec_w1: bfloat16 [2, 1024, 3072], replicated
- dec_w2: bfloat16 [2, 3072, 1024], replicated
Outputs:
- output: bfloat16 [512, 64, 1024], P(('data', 'stage'))
All inputs are finite; a program needn't handle non-finite values.
Results may differ from the reference program's by a relative error of at most 0.0121753.
Values are sent between devices in bfloat16 or wider.
A program may use at most 768 MiB of HBM per device.

```python
import jax
import jax.numpy as jnp
from jax import lax

D = 1024
HEADS = 16
KV_HEADS = 8
HEAD = 128
FF = 3072
S_ENC = 256
S_DEC = 64
N_SEQ = 512
L_ENC = 2
L_DEC = 2

REP = HEADS // KV_HEADS


def weight(weight_key, shape, fan_in):
    return (jax.random.normal(weight_key, shape, jnp.float32) * fan_in ** -0.5).astype(jnp.bfloat16)


def structured(key_set, length):
    trend = jnp.linspace(-1.0, 1.0, length)[None, :, None]
    common = jax.random.normal(key_set[0], (N_SEQ, 1, D), jnp.float32)
    slope = jax.random.normal(key_set[1], (N_SEQ, 1, D), jnp.float32)
    noise = jax.random.normal(key_set[2], (N_SEQ, length, D), jnp.float32)
    return (0.5 * common + 0.8 * trend * slope + 0.4 * noise).astype(jnp.bfloat16)


def setup_inputs(seed: int = 0, part: int = 0) -> dict:
    part_keys = jax.random.split(jax.random.fold_in(jax.random.key(seed), part), 7)
    weight_keys = jax.random.split(jax.random.key(seed + 1), 11)
    lengths = jax.random.randint(part_keys[6], (N_SEQ,), S_ENC // 4, S_ENC + 1, jnp.int32)
    lengths = lengths.at[0].set(S_ENC)
    return {
        "x_enc": structured(part_keys[0:3], S_ENC),
        "enc_len": lengths,
        "y": structured(part_keys[3:6], S_DEC),
        "enc_wqkv": weight(weight_keys[0], (L_ENC, D, 3, HEADS, HEAD), D),
        "enc_wo": weight(weight_keys[1], (L_ENC, HEADS, HEAD, D), HEADS * HEAD),
        "enc_w1": weight(weight_keys[2], (L_ENC, D, FF), D),
        "enc_w2": weight(weight_keys[3], (L_ENC, FF, D), FF),
        "dec_wqkv": weight(weight_keys[4], (L_DEC, D, 3, HEADS, HEAD), D),
        "dec_wo": weight(weight_keys[5], (L_DEC, HEADS, HEAD, D), HEADS * HEAD),
        "cross_wq": weight(weight_keys[6], (L_DEC, D, KV_HEADS, REP, HEAD), D),
        "cross_wkv": weight(weight_keys[7], (L_DEC, D, 2, KV_HEADS, HEAD), D),
        "cross_wo": weight(weight_keys[8], (L_DEC, KV_HEADS, REP, HEAD, D), HEADS * HEAD),
        "dec_w1": weight(weight_keys[9], (L_DEC, D, FF), D),
        "dec_w2": weight(weight_keys[10], (L_DEC, FF, D), FF),
    }


def rms_norm(inputs):
    wide = inputs.astype(jnp.float32)
    return (wide * lax.rsqrt(jnp.mean(wide * wide, axis=-1, keepdims=True) + 1e-6)).astype(jnp.bfloat16)


def attend(query, keys, values, valid):
    scores = jnp.einsum("qgrd,kgd->grqk", query.astype(jnp.float32), keys.astype(jnp.float32)) * HEAD ** -0.5
    attn_probs = jax.nn.softmax(jnp.where(valid, scores, -1e30), axis=-1).astype(jnp.bfloat16)
    return jnp.einsum("grqk,kgd->qgrd", attn_probs.astype(jnp.float32), values.astype(jnp.float32)).astype(jnp.bfloat16)


def self_block(state, w_qkv, w_out, valid):
    proj_qkv = jnp.einsum("sd,dthe->tshe", rms_norm(state).astype(jnp.float32), w_qkv.astype(jnp.float32)).astype(jnp.bfloat16)
    mixed = attend(proj_qkv[0][:, :, None, :], proj_qkv[1], proj_qkv[2], valid)
    update = jnp.einsum("shre,hev->sv", mixed.astype(jnp.float32), w_out.astype(jnp.float32))
    return (state.astype(jnp.float32) + update).astype(jnp.bfloat16)


def ffn_block(state, w_in, w_out):
    hidden = jax.nn.gelu(jnp.dot(rms_norm(state), w_in, preferred_element_type=jnp.float32)).astype(jnp.bfloat16)
    return (state.astype(jnp.float32) + jnp.dot(hidden, w_out, preferred_element_type=jnp.float32)).astype(jnp.bfloat16)


def reference(x_enc, enc_len, y, enc_wqkv, enc_wo, enc_w1, enc_w2, dec_wqkv, dec_wo, cross_wq, cross_wkv, cross_wo, dec_w1, dec_w2):
    def encode_one(pair):
        state = pair[0]
        valid = jnp.arange(S_ENC) < pair[1]
        for layer in range(L_ENC):
            state = self_block(state, enc_wqkv[layer], enc_wo[layer], valid)
            state = ffn_block(state, enc_w1[layer], enc_w2[layer])
        return rms_norm(state)

    enc_states = lax.map(encode_one, (x_enc, enc_len))
    partner_out = jnp.roll(enc_states, N_SEQ // 2, axis=0)
    partner_len = jnp.roll(enc_len, N_SEQ // 2, axis=0)
    positions = jnp.arange(S_DEC)
    causal = positions[None, :] <= positions[:, None]

    def decode_one(triple):
        state, enc_seq, length = triple
        keep = jnp.arange(S_ENC) < length
        for layer in range(L_DEC):
            state = self_block(state, dec_wqkv[layer], dec_wo[layer], causal)
            query = jnp.einsum("sd,dgre->sgre", rms_norm(state).astype(jnp.float32), cross_wq[layer].astype(jnp.float32)).astype(jnp.bfloat16)
            key_vals = jnp.einsum("sd,dtge->tsge", enc_seq.astype(jnp.float32), cross_wkv[layer].astype(jnp.float32)).astype(jnp.bfloat16)
            mixed = attend(query, key_vals[0], key_vals[1], keep)
            update = jnp.einsum("sgre,grev->sv", mixed.astype(jnp.float32), cross_wo[layer].astype(jnp.float32))
            state = (state.astype(jnp.float32) + update).astype(jnp.bfloat16)
            state = ffn_block(state, dec_w1[layer], dec_w2[layer])
        return state

    return lax.map(decode_one, (y, partner_out, partner_len))
```

```python
import functools
import math

import jax
import jax.numpy as jnp
from jax import lax
from jax.experimental import pallas as pl
from jax.experimental.pallas import tpu as pltpu
from jax.sharding import PartitionSpec as P

NEG = -1e30
VMEM_LIMIT = 60 * 1024 * 1024
ENC_STEP = 2
DEC_STEP = 4


def rms_norm(inputs):
    wide = inputs.astype(jnp.float32)
    return (wide * lax.rsqrt(jnp.mean(wide * wide, axis=-1, keepdims=True) + 1e-6)).astype(jnp.bfloat16)


def dot(left, right):
    return jnp.dot(left, right, preferred_element_type=jnp.float32)


def attend(query, keys, values, valid):
    scores = lax.dot_general(query, keys, (((1,), (1,)), ((), ())), preferred_element_type=jnp.float32)
    scores = jnp.where(valid, scores, NEG)
    top = jnp.max(scores, axis=-1, keepdims=True)
    weights = jnp.exp2((scores - top) * (query.shape[-1] ** -0.5 * math.log2(math.e)))
    probs = (weights * (1.0 / jnp.sum(weights, axis=-1, keepdims=True))).astype(jnp.bfloat16)
    return dot(probs, values).astype(jnp.bfloat16)


def gelu(x):
    half = 0.5 * x
    root = math.sqrt(2.0 / math.pi)
    return (half + half * jnp.tanh(x * (root + (root * 0.044715) * (x * x)))).astype(jnp.bfloat16)


def ffn(state, w1, w2, hidden, chunk):
    normed = rms_norm(state)
    width = w1.shape[1]
    for start in range(0, width, chunk):
        cols = pl.ds(start, chunk)
        hidden[:, cols] = gelu(dot(normed, w1[:, cols]))
    return (state.astype(jnp.float32) + dot(hidden[...], w2[...])).astype(jnp.bfloat16)


def weight_copies(layer, sources, targets, sems):
    return [
        pltpu.make_async_copy(source.at[layer], target, sems.at[i])
        for i, (source, target) in enumerate(zip(sources, targets))
    ]


def enc_kernel(layer, chunk, len_ref, qkv_ref, x_ref, wo_hbm, w1_hbm, w2_hbm, out_ref, wo, w1, w2, mixed, state_s, hidden, sems):
    step = pl.program_id(0)
    first = step == 0
    copies = weight_copies(layer, (wo_hbm, w1_hbm, w2_hbm), (wo, w1, w2), sems)

    @pl.when(first)
    def _():
        for copy in copies:
            copy.start()

    seqs, _, heads, length, head = qkv_ref.shape

    def one(b, carry):
        rows = pl.ds(pl.multiple_of(b * length, length), length)
        valid = lax.broadcasted_iota(jnp.int32, (1, length), 1) < len_ref[step * seqs + b]
        for h in range(heads):
            mixed[rows, h * head:(h + 1) * head] = attend(qkv_ref[b, 0, h], qkv_ref[b, 1, h], qkv_ref[b, 2, h], valid)
        return carry

    lax.fori_loop(0, seqs, one, 0)

    @pl.when(first)
    def _():
        copies[0].wait()

    x = x_ref[...].reshape(seqs * length, x_ref.shape[-1])
    state_s[...] = (x.astype(jnp.float32) + dot(mixed[...], wo[...])).astype(jnp.bfloat16)

    @pl.when(first)
    def _():
        copies[1].wait()
        copies[2].wait()

    out_ref[...] = ffn(state_s[...], w1, w2, hidden, chunk).reshape(out_ref.shape)


def dec_kernel(layer, chunk, len_ref, qkv_ref, y_ref, kv_ref, wo_hbm, wq_hbm, cwo_hbm, w1_hbm, w2_hbm, out_ref,
               wo, wq, cwo, w1, w2, mixed, query_s, state_s, hidden, sems):
    step = pl.program_id(0)
    first = step == 0
    copies = weight_copies(layer, (wo_hbm, wq_hbm, cwo_hbm, w1_hbm, w2_hbm), (wo, wq, cwo, w1, w2), sems)

    @pl.when(first)
    def _():
        for copy in copies:
            copy.start()

    seqs, _, heads, length, head = qkv_ref.shape
    rows = seqs * length
    groups, keys_len = kv_ref.shape[3], kv_ref.shape[4]
    rep = heads // groups
    row = lax.broadcasted_iota(jnp.int32, (rows, rows), 0)
    col = lax.broadcasted_iota(jnp.int32, (rows, rows), 1)
    causal = (col <= row) & (col >= row - lax.rem(row, length))
    for h in range(heads):
        query, keys, values = (qkv_ref[:, t, h].reshape(rows, head) for t in range(3))
        mixed[:, h * head:(h + 1) * head] = attend(query, keys, values, causal)

    @pl.when(first)
    def _():
        copies[0].wait()
        copies[1].wait()

    y = y_ref[...].reshape(rows, y_ref.shape[-1])
    state_s[...] = (y.astype(jnp.float32) + dot(mixed[...], wo[...])).astype(jnp.bfloat16)
    query_s[...] = dot(rms_norm(state_s[...]), wq[...]).astype(jnp.bfloat16)

    for b in range(seqs):
        valid = lax.broadcasted_iota(jnp.int32, (1, keys_len), 1) < len_ref[step * seqs + b]
        at = slice(b * length, (b + 1) * length)
        for g in range(groups):
            spans = [slice((g * rep + r) * head, (g * rep + r + 1) * head) for r in range(rep)]
            query = jnp.concatenate([query_s[at, span] for span in spans], axis=0)
            result = attend(query, kv_ref[0, b, 0, g], kv_ref[0, b, 1, g], valid)
            for r, span in enumerate(spans):
                mixed[at, span] = result[r * length:(r + 1) * length]

    @pl.when(first)
    def _():
        for copy in copies[2:]:
            copy.wait()

    state_s[...] = (state_s[...].astype(jnp.float32) + dot(mixed[...], cwo[...])).astype(jnp.bfloat16)
    out_ref[...] = ffn(state_s[...], w1, w2, hidden, chunk).reshape(out_ref.shape)


def call(kernel, step_seqs, lens, qkv, state, others, weights, layer, flops):
    n_seq, _, heads, length, head = qkv.shape
    d = state.shape[-1]
    width = weights[-1].shape[1]
    seqs = math.gcd(step_seqs, n_seq)
    rows = seqs * length
    block = lambda *tail: pl.BlockSpec((seqs,) + tail, lambda i, lens: (i,) + (0,) * len(tail))
    scratch = [pltpu.VMEM(w.shape[1:], w.dtype) for w in weights]
    scratch.append(pltpu.VMEM((rows, heads * head), jnp.bfloat16))
    if others:
        scratch.append(pltpu.VMEM((rows, heads * head), jnp.bfloat16))
    scratch += [pltpu.VMEM((rows, d), jnp.bfloat16), pltpu.VMEM((rows, width), jnp.bfloat16)]
    scratch.append(pltpu.SemaphoreType.DMA((len(weights),)))
    other_specs = [
        pl.BlockSpec((1, seqs) + o.shape[2:], lambda i, lens: (layer, i, 0, 0, 0, 0)) for o in others
    ]
    moved = 2 * sum(a.size for a in (qkv, state, state)) + sum(2 * w.size // w.shape[0] for w in weights)
    return pl.pallas_call(
        functools.partial(kernel, layer, min(width, 1024)),
        out_shape=jax.ShapeDtypeStruct(state.shape, state.dtype),
        grid_spec=pltpu.PrefetchScalarGridSpec(
            num_scalar_prefetch=1,
            grid=(n_seq // seqs,),
            in_specs=[block(3, heads, length, head), block(length, d)] + other_specs
            + [pl.BlockSpec(memory_space=pl.ANY)] * len(weights),
            out_specs=block(length, d),
            scratch_shapes=scratch,
        ),
        compiler_params=pltpu.CompilerParams(dimension_semantics=("arbitrary",), vmem_limit_bytes=VMEM_LIMIT),
        cost_estimate=pl.CostEstimate(flops=flops, bytes_accessed=moved, transcendentals=0),
    )(lens, qkv, state, *others, *weights)


def project_qkv(state, w_qkv):
    return jnp.einsum("bsd,dthe->bthse", rms_norm(state), w_qkv, preferred_element_type=jnp.float32).astype(jnp.bfloat16)


def merge_heads(w):
    return w.reshape(w.shape[0], -1, w.shape[-1])


def solution(mesh):
    stages = mesh.shape["stage"]
    swap = [(source, (source + stages // 2) % stages) for source in range(stages)]
    rows = P(("data", "stage"))
    whole = P()

    def body(x_enc, enc_len, y, enc_wqkv, enc_wo, enc_w1, enc_w2, dec_wqkv, dec_wo, cross_wq, cross_wkv, cross_wo, dec_w1, dec_w2):
        guest = lax.ppermute(y, "stage", swap)
        d = x_enc.shape[-1]
        enc_weights = [merge_heads(enc_wo), enc_w1, enc_w2]
        dec_weights = [merge_heads(dec_wo), cross_wq.reshape(cross_wq.shape[0], d, -1), merge_heads(cross_wo), dec_w1, dec_w2]
        macs = lambda ws: sum(w.size // w.shape[0] for w in ws)
        state = x_enc
        for layer in range(enc_wqkv.shape[0]):
            qkv = project_qkv(state, enc_wqkv[layer])
            flops = 2 * state.size // d * (macs(enc_weights) + 2 * qkv.shape[2] * qkv.shape[4] * x_enc.shape[1])
            state = call(enc_kernel, ENC_STEP, enc_len, qkv, state, [], enc_weights, layer, flops)
        kv_all = jnp.einsum("bsd,ldtge->lbtgse", rms_norm(state), cross_wkv, preferred_element_type=jnp.float32).astype(jnp.bfloat16)
        state = guest
        for layer in range(dec_wqkv.shape[0]):
            qkv = project_qkv(state, dec_wqkv[layer])
            flops = 2 * state.size // d * (macs(dec_weights) + 4 * qkv.shape[2] * qkv.shape[4] * x_enc.shape[1])
            state = call(dec_kernel, DEC_STEP, enc_len, qkv, state, [kv_all], dec_weights, layer, flops)
        return lax.ppermute(state, "stage", swap)

    return jax.shard_map(body, mesh=mesh, in_specs=(rows, rows, rows) + (whole,) * 11, out_specs=rows, check_vma=False)
```

```python
import functools
import math

import jax
import jax.numpy as jnp
from jax import lax
from jax.experimental import pallas as pl
from jax.experimental.pallas import tpu as pltpu
from jax.sharding import PartitionSpec as P

NEG = -1e30
VMEM_LIMIT = 67043328
ENC_STEP = 2
DEC_STEP = 4


def rms_norm(inputs):
    wide = inputs.astype(jnp.float32)
    return (wide * lax.rsqrt(jnp.mean(wide * wide, axis=-1, keepdims=True) + 1e-6)).astype(jnp.bfloat16)


def dot(left, right):
    return jnp.dot(left, right, preferred_element_type=jnp.float32)


def attend(query, keys, values, valid):
    scores = lax.dot_general(query, keys, (((1,), (1,)), ((), ())), preferred_element_type=jnp.float32)
    scores = jnp.where(valid, scores, NEG)
    top = jnp.max(scores, axis=-1, keepdims=True)
    weights = jnp.exp2((scores - top) * (query.shape[-1] ** -0.5 * math.log2(math.e)))
    probs = (weights * (1.0 / jnp.sum(weights, axis=-1, keepdims=True))).astype(jnp.bfloat16)
    return dot(probs, values).astype(jnp.bfloat16)


def gelu(x):
    half = 0.5 * x
    root = math.sqrt(2.0 / math.pi)
    return (half + half * jnp.tanh(x * (root + (root * 0.044715) * (x * x)))).astype(jnp.bfloat16)


def ffn(state, w1, w2, hidden, chunk):
    normed = rms_norm(state)
    width = w1.shape[1]
    for start in range(0, width, chunk):
        cols = pl.ds(start, chunk)
        hidden[:, cols] = gelu(dot(normed, w1[:, cols]))
    return (state.astype(jnp.float32) + dot(hidden[...], w2[...])).astype(jnp.bfloat16)


def weight_copies(layer, sources, targets, sems):
    return [
        pltpu.make_async_copy(source.at[layer], target, sems.at[i])
        for i, (source, target) in enumerate(zip(sources, targets))
    ]


def enc_kernel(layer, chunk, begin, len_ref, qkv_ref, x_ref, wo_hbm, w1_hbm, w2_hbm, out_ref, norm_ref, wo, w1, w2, mixed, state_s, hidden, sems):
    step = pl.program_id(0)
    first = step == 0
    copies = weight_copies(layer, (wo_hbm, w1_hbm, w2_hbm), (wo, w1, w2), sems)

    @pl.when(first)
    def _():
        for copy in copies:
            copy.start()

    seqs, _, heads, length, head = qkv_ref.shape

    def one(b, carry):
        rows = pl.ds(pl.multiple_of(b * length, length), length)
        valid = lax.broadcasted_iota(jnp.int32, (1, length), 1) < len_ref[(begin + step) * seqs + b]
        for h in range(heads):
            mixed[rows, h * head:(h + 1) * head] = attend(qkv_ref[b, 0, h], qkv_ref[b, 1, h], qkv_ref[b, 2, h], valid)
        return carry

    lax.fori_loop(0, seqs, one, 0)

    @pl.when(first)
    def _():
        copies[0].wait()

    x = x_ref[...].reshape(seqs * length, x_ref.shape[-1])
    state_s[...] = (x.astype(jnp.float32) + dot(mixed[...], wo[...])).astype(jnp.bfloat16)

    @pl.when(first)
    def _():
        copies[1].wait()
        copies[2].wait()

    result = ffn(state_s[...], w1, w2, hidden, chunk)
    out_ref[...] = result.reshape(out_ref.shape)
    norm_ref[...] = rms_norm(result).reshape(out_ref.shape)


def dec_kernel(layer, chunk, begin, len_ref, qkv_ref, y_ref, kv_ref, wo_hbm, wq_hbm, cwo_hbm, w1_hbm, w2_hbm, out_ref, norm_ref,
               wo, wq, cwo, w1, w2, mixed, query_s, state_s, hidden, sems):
    step = pl.program_id(0)
    first = step == 0
    copies = weight_copies(layer, (wo_hbm, wq_hbm, cwo_hbm, w1_hbm, w2_hbm), (wo, wq, cwo, w1, w2), sems)

    @pl.when(first)
    def _():
        for copy in copies:
            copy.start()

    seqs, _, heads, length, head = qkv_ref.shape
    rows = seqs * length
    groups, keys_len = kv_ref.shape[3], kv_ref.shape[4]
    rep = heads // groups
    row = lax.broadcasted_iota(jnp.int32, (rows, rows), 0)
    col = lax.broadcasted_iota(jnp.int32, (rows, rows), 1)
    causal = (col <= row) & (col >= row - lax.rem(row, length))
    for h in range(heads):
        query, keys, values = (qkv_ref[:, t, h].reshape(rows, head) for t in range(3))
        mixed[:, h * head:(h + 1) * head] = attend(query, keys, values, causal)

    @pl.when(first)
    def _():
        copies[0].wait()
        copies[1].wait()

    y = y_ref[...].reshape(rows, y_ref.shape[-1])
    state_s[...] = (y.astype(jnp.float32) + dot(mixed[...], wo[...])).astype(jnp.bfloat16)
    query_s[...] = dot(rms_norm(state_s[...]), wq[...]).astype(jnp.bfloat16)

    for b in range(seqs):
        valid = lax.broadcasted_iota(jnp.int32, (1, keys_len), 1) < len_ref[(begin + step) * seqs + b]
        at = slice(b * length, (b + 1) * length)
        for g in range(groups):
            spans = [slice((g * rep + r) * head, (g * rep + r + 1) * head) for r in range(rep)]
            query = jnp.concatenate([query_s[at, span] for span in spans], axis=0)
            answer = attend(query, kv_ref[0, b, 0, g], kv_ref[0, b, 1, g], valid)
            for r, span in enumerate(spans):
                mixed[at, span] = answer[r * length:(r + 1) * length]

    @pl.when(first)
    def _():
        for copy in copies[2:]:
            copy.wait()

    state_s[...] = (state_s[...].astype(jnp.float32) + dot(mixed[...], cwo[...])).astype(jnp.bfloat16)
    result = ffn(state_s[...], w1, w2, hidden, chunk)
    out_ref[...] = result.reshape(out_ref.shape)
    norm_ref[...] = rms_norm(result).reshape(out_ref.shape)


def call(kernel, step_seqs, lens, qkv, state, others, weights, layer, flops, begin=0, steps=None):
    n_seq, _, heads, length, head = qkv.shape
    d = state.shape[-1]
    width = weights[-1].shape[1]
    seqs = math.gcd(step_seqs, n_seq)
    rows = seqs * length
    steps = n_seq // seqs if steps is None else steps
    block = lambda *tail: pl.BlockSpec((seqs,) + tail, lambda i, lens: (begin + i,) + (0,) * len(tail))
    result = pl.BlockSpec((seqs, length, d), lambda i, lens: (i, 0, 0))
    out = jax.ShapeDtypeStruct((steps * seqs, length, d), state.dtype)
    scratch = [pltpu.VMEM(w.shape[1:], w.dtype) for w in weights]
    scratch.append(pltpu.VMEM((rows, heads * head), jnp.bfloat16))
    if others:
        scratch.append(pltpu.VMEM((rows, heads * head), jnp.bfloat16))
    scratch += [pltpu.VMEM((rows, d), jnp.bfloat16), pltpu.VMEM((rows, width), jnp.bfloat16)]
    scratch.append(pltpu.SemaphoreType.DMA((len(weights),)))
    other_specs = [
        pl.BlockSpec((1, seqs) + o.shape[2:], lambda i, lens: (layer, begin + i, 0, 0, 0, 0)) for o in others
    ]
    moved = 2 * sum(a.size for a in (qkv, state, state)) + sum(2 * w.size // w.shape[0] for w in weights)
    return pl.pallas_call(
        functools.partial(kernel, layer, min(width, 1024), begin),
        out_shape=(out, out),
        grid_spec=pltpu.PrefetchScalarGridSpec(
            num_scalar_prefetch=1,
            grid=(steps,),
            in_specs=[block(3, heads, length, head), block(length, d)] + other_specs
            + [pl.BlockSpec(memory_space=pl.ANY)] * len(weights),
            out_specs=(result, result),
            scratch_shapes=scratch,
        ),
        compiler_params=pltpu.CompilerParams(dimension_semantics=("arbitrary",), vmem_limit_bytes=VMEM_LIMIT),
        cost_estimate=pl.CostEstimate(flops=flops, bytes_accessed=moved, transcendentals=0),
    )(lens, qkv, state, *others, *weights)


def project_qkv(normed, w_qkv):
    return jnp.einsum("bsd,dthe->bthse", normed, w_qkv, preferred_element_type=jnp.float32).astype(jnp.bfloat16)


def merge_heads(w):
    return w.reshape(w.shape[0], -1, w.shape[-1])


def solution(mesh):
    stages = mesh.shape["stage"]
    swap = [(source, (source + stages // 2) % stages) for source in range(stages)]
    rows = P(("data", "stage"))
    whole = P()

    def body(x_enc, enc_len, y, enc_wqkv, enc_wo, enc_w1, enc_w2, dec_wqkv, dec_wo, cross_wq, cross_wkv, cross_wo, dec_w1, dec_w2):
        guest = lax.ppermute(y, "stage", swap)
        d = x_enc.shape[-1]
        enc_weights = [merge_heads(enc_wo), enc_w1, enc_w2]
        dec_weights = [merge_heads(dec_wo), cross_wq.reshape(cross_wq.shape[0], d, -1), merge_heads(cross_wo), dec_w1, dec_w2]
        macs = lambda ws: sum(w.size // w.shape[0] for w in ws)
        state, normed = x_enc, rms_norm(x_enc)
        for layer in range(enc_wqkv.shape[0]):
            qkv = project_qkv(normed, enc_wqkv[layer])
            flops = 2 * state.size // d * (macs(enc_weights) + 2 * qkv.shape[2] * qkv.shape[4] * x_enc.shape[1])
            state, normed = call(enc_kernel, ENC_STEP, enc_len, qkv, state, [], enc_weights, layer, flops)
        kv_all = jnp.einsum("bsd,ldtge->lbtgse", normed, cross_wkv, preferred_element_type=jnp.float32).astype(jnp.bfloat16)
        state, normed = guest, rms_norm(guest)
        last = dec_wqkv.shape[0] - 1
        total = y.shape[0] // math.gcd(DEC_STEP, y.shape[0])
        half, quarter = total - total // 2, total // 4
        pieces = [(0, half), (half, total - half - quarter), (total - quarter, quarter)]
        for layer in range(last + 1):
            qkv = project_qkv(normed, dec_wqkv[layer])
            flops = 2 * state.size // d * (macs(dec_weights) + 4 * qkv.shape[2] * qkv.shape[4] * x_enc.shape[1])
            run = functools.partial(call, dec_kernel, DEC_STEP, enc_len, qkv, state, [kv_all], dec_weights, layer)
            if layer < last:
                state, normed = run(flops)
        sent = []
        for begin, steps in pieces:
            if steps:
                sent.append(lax.ppermute(run(flops * steps // (64 * total), begin, steps)[0], "stage", swap))
        return jnp.concatenate(sent, axis=0)

    return jax.shard_map(body, mesh=mesh, in_specs=(rows, rows, rows) + (whole,) * 11, out_specs=rows, check_vma=False)
```
